32 devices in a mesh: dp: 4 (over y, core), tensor: 8 (over z, x).
Axes of the slice: x: 2, y: 2, z: 4, core: 2. Of those that a mesh axis runs over, the one named last changes fastest.
Arguments:
- grads: bfloat16 [4, 2, 7168, 2048], P('dp', None, 'tensor'), may hold values from -6 to 6
- master: float32 [2, 7168, 2048], P(None, 'dp', 'tensor'), may hold values from -0.0625 to 0.0625
- moment1: float32 [2, 7168, 2048], P(None, 'dp', 'tensor'), may hold values from -3 to 3
- moment2: float32 [2, 7168, 2048], P(None, 'dp', 'tensor'), may hold values from 1 to 30
- tokens: bfloat16 [1024, 7168], P('dp'), may hold values from -6 to 6
- route: int32 [512], P('dp'), may hold values from 0 to 255, as said below
Outputs:
- new_master: float32 [2, 7168, 2048], P(None, 'dp', 'tensor')
- new_moment1: float32 [2, 7168, 2048], P(None, 'dp', 'tensor')
- new_moment2: float32 [2, 7168, 2048], P(None, 'dp', 'tensor')
- rollout: bfloat16 [2, 7168, 2048], P(None, None, 'tensor')
- hidden: bfloat16 [512, 2048], P('dp', 'tensor')
The draws below stay inside these ranges and needn't reach their ends.
Inputs may be any that keep to these rules, and one draw needn't show every extreme that they name: route[i] indexes one of the 256 tokens of the data rank that holds routed row i; within one data rank's 128 routed rows no token appears twice.
All inputs are finite; a program needn't handle non-finite values.
Results may differ from the reference program's by a relative error of at most 0.019.
Values may be sent and summed in bfloat16 or wider, within the bound.
A program may use at most 128 MiB of HBM per device.

```python
import math
import jax
import jax.numpy as jnp
from jax import lax

D = 7168
H = 2048
TOK_DEV = 256
ROUTED_DEV = 128
TOKENS = 1024
ROUTED = 512
N_DP = 4


def draw_route(key, part):
    rank_keys = jax.random.split(key, ROUTED // ROUTED_DEV)

    def one_rank(rank_key):
        order = jax.random.permutation(rank_key, TOK_DEV)
        return order[:ROUTED_DEV]
    chosen = jax.vmap(one_rank)(rank_keys)
    return chosen.reshape(ROUTED).astype(jnp.int32)


def spiked(entries, key, source, target, parts, factor):
    owner, partner = [(jnp.arange(entries.shape[axis_at]) // (entries.shape[axis_at] // parts)).reshape([-1 if axis == axis_at else 1 for axis in range(entries.ndim)]) for axis_at in (source, target)]
    chosen = jax.random.permutation(key, parts)[partner]
    strong = (owner == chosen) | (owner == (partner + parts // 2) % parts)
    return jnp.where(strong, factor * entries, entries)


def shard_levels(stream_key, shape, cuts, least, largest):
    loudness = 1.0
    for axis_at, shards_of in cuts:
        draws = jax.random.uniform(jax.random.fold_in(jax.random.fold_in(stream_key, 6), axis_at), (shards_of,), jnp.float32, least / len(cuts), largest / len(cuts))
        loudness = loudness * jnp.repeat(jnp.exp(draws), shape[axis_at] // shards_of).reshape((-1,) + (1,) * (len(shape) - 1 - axis_at))
    return loudness


def centred(rng, dims, width, reach, shards=(), held_as=jnp.bfloat16):
    array = jax.random.normal(rng, dims, jnp.float32) * width
    if len(shards) > 0:
        array = shard_levels(rng, dims, shards, -0.22, 0.18) * array
    return jnp.clip(array, min=-reach, max=reach).astype(held_as)


def noise_with(stream_key, extent, deviation, limit, cuts, heavy, kind=jnp.bfloat16):
    values = deviation * jax.random.normal(stream_key, extent, jnp.float32)
    if cuts:
        values = values * shard_levels(stream_key, extent, cuts, -0.22, 0.18)
    return jnp.clip(spiked(values, jax.random.fold_in(stream_key, 3), *heavy), -limit, limit).astype(kind)


def setup_inputs(seed: int = 0) -> dict:
    key_list = jax.random.split(jax.random.key(seed), 7)
    grads = noise_with(key_list[0], (N_DP, 2, D, H), 1.0, 6.0, ((0, 4), (2, 8)), (0, 2, 4, 2.0))
    master = centred(key_list[1], (2, D, H), D ** -0.5, 0.0625, ((1, 4), (2, 8)), jnp.float32)
    moment1 = centred(key_list[2], (2, D, H), 0.5, 3.0, ((1, 4), (2, 8)), jnp.float32)
    moment2 = jnp.clip(jnp.exp(math.log(30.0) - 3.4011974 * jax.random.uniform(key_list[3], (2, D, H), jnp.float32) ** shard_levels(key_list[3], (2, D, H), ((1, 4), (2, 8)), -0.2, 0.2)), 1.0, 30.0)
    tokens = centred(key_list[4], (TOKENS, D), 1.0, 6.0, ((0, 4),))
    route = draw_route(jax.random.fold_in(key_list[6], 71), 0)
    return {"grads": grads, "master": master, "moment1": moment1, "moment2": moment2, "tokens": tokens, "route": route}


def reference(grads, master, moment1, moment2, tokens, route):

    def accumulate(carry, piece):
        return (carry + piece.astype(jnp.float32), None)
    start = jnp.zeros(master.shape, jnp.float32)
    grad_total, _ = lax.scan(accumulate, start, grads)
    new_moment1 = 0.9 * moment1 + 0.1 * grad_total
    new_moment2 = 0.95 * moment2 + 0.05 * grad_total * grad_total
    first_fix = 1.0 - 0.9 ** 10
    second_fix = 1.0 - 0.95 ** 10
    step_size = new_moment1 / first_fix / (jnp.sqrt(new_moment2 / second_fix) + 1e-08) + 0.1 * master
    new_master = master - 0.003 * step_size
    rollout = new_master.astype(jnp.bfloat16)
    block = jnp.arange(ROUTED, dtype=jnp.int32) // ROUTED_DEV
    row_index = (block * TOK_DEV + route).astype(jnp.int32)
    picked = jnp.take(tokens, row_index, axis=0)
    gate_out = jnp.dot(picked, rollout[0], preferred_element_type=jnp.float32)
    up_out = jnp.dot(picked, rollout[1], preferred_element_type=jnp.float32)
    hidden = (jax.nn.silu(gate_out) * up_out).astype(jnp.bfloat16)
    return (new_master, new_moment1, new_moment2, rollout, hidden)
```

```python
import functools

import jax
import jax.numpy as jnp
from jax import lax
from jax.experimental import pallas as pl
from jax.experimental.pallas import tpu as pltpu
from jax.sharding import PartitionSpec as P

MESH = pl.DeviceIdType.MESH
LANES = 128
AHEAD = 2


def body(grads, master, moment1, moment2, tokens, route):
    tensor_count = lax.axis_size("tensor")
    rank_count = lax.axis_size("dp")
    grad_local = grads[0]
    rows_tensor = grad_local.shape[1]
    hidden_width = grad_local.shape[2]
    col_width = hidden_width // tensor_count
    slab = rows_tensor // rank_count
    summed = lax.psum_scatter(grad_local, "dp", scatter_dimension=1, tiled=True).astype(jnp.float32)
    pieces = summed.reshape(2, slab, tensor_count, col_width)
    spread = lax.all_to_all(
        pieces.astype(jnp.bfloat16), "tensor", split_axis=2, concat_axis=1, tiled=True
    ).astype(pieces.dtype)
    spread = spread.reshape(2, rank_count, tensor_count // rank_count, slab, col_width)
    owned = lax.all_to_all(
        spread.astype(jnp.bfloat16), "dp", split_axis=1, concat_axis=3, tiled=True
    ).astype(spread.dtype)
    grad_total = owned.reshape(2, rows_tensor * tensor_count // rank_count, col_width)
    new_moment1 = 0.9 * moment1 + 0.1 * grad_total
    new_moment2 = 0.95 * moment2 + 0.05 * grad_total * grad_total
    first_fix = 1.0 - 0.9**10
    second_fix = 1.0 - 0.95**10
    step_size = (
        new_moment1 / first_fix / (jnp.sqrt(new_moment2 / second_fix) + 1e-08) + 0.1 * master
    )
    new_master = master - 0.003 * step_size
    rollout_shard = new_master.astype(jnp.bfloat16)
    replicated = lax.all_gather(rollout_shard, "dp", axis=1, tiled=True)
    picked = jnp.take(tokens, route, axis=0)
    both = jnp.einsum("rd,kdh->rkh", picked, replicated, preferred_element_type=jnp.float32)
    hidden = (jax.nn.silu(both[:, 0, :]) * both[:, 1, :]).astype(jnp.bfloat16)
    return (new_master, new_moment1, new_moment2, replicated, hidden)


def kernel(
    tensor_count,
    grads,
    states,
    tokens,
    route,
    outs,
    rollout,
    hidden,
    mine,
    theirs,
    land,
    crossed,
    held,
    roll,
    token_rows,
    picked,
    acc,
    load_sem,
    core_send,
    core_recv,
    state_sem,
    token_sem,
    spread_send,
    spread_recv,
    cross_send,
    cross_recv,
    near_send,
    near_recv,
    far_send,
    far_recv,
    relay_send,
    relay_recv,
    out_sem,
    roll_sem,
):
    rank = lax.axis_index("dp")
    place = lax.axis_index("tensor")
    row, core = rank // 2, rank % 2
    near = row * 2 + 1 - core
    far = (1 - row) * 2 + core
    across = (1 - row) * 2 + 1 - core
    subs = land.shape[1]
    slab = mine.shape[0]
    width = land.shape[4]
    chunk = picked.shape[2] // tensor_count
    steps = slab // chunk
    owner, sub = place // subs, place % subs
    owner_row, owner_core = owner // 2, owner % 2
    side = (owner_row + row) % 2

    def rows(step):
        return pl.ds(pl.multiple_of(step * chunk, chunk), chunk)

    def remote(source, target, send, recv, to_rank, to_place):
        return pltpu.make_async_remote_copy(
            src_ref=source,
            dst_ref=target,
            send_sem=send,
            recv_sem=recv,
            device_id=(to_rank, to_place),
            device_id_type=MESH,
        )

    def load(step):
        return pltpu.make_async_copy(
            grads.at[0, core, rows(step)], mine.at[rows(step)], load_sem.at[step]
        )

    def swap(step):
        return remote(
            grads.at[0, 1 - core, rows(step)],
            theirs.at[rows(step)],
            core_send.at[step],
            core_recv.at[step],
            near,
            place,
        )

    def state(which, step):
        return pltpu.make_async_copy(
            states[which].at[:, :, rows(step)],
            held.at[which, :, :, rows(step)],
            state_sem.at[which * steps + step],
        )

    def state_out(which, step):
        return pltpu.make_async_copy(
            held.at[which, :, :, rows(step)],
            outs[which].at[:, :, rows(step)],
            out_sem.at[which * steps + step],
        )

    def landing(step, part, piece, half):
        return ((step * 2 + part) * subs + piece) * 2 + half

    def spread(step, offset):
        goal = (place + offset) % tensor_count
        return remote(
            mine.at[rows(step), pl.ds(pl.multiple_of(goal * width, width), width)],
            land.at[side, sub, core, rows(step)],
            spread_send.at[step * tensor_count + offset],
            spread_recv.at[landing(step, side, sub, core)],
            row * 2 + owner_core,
            goal,
        )

    def spread_self(step):
        return pltpu.make_async_copy(
            mine.at[rows(step), pl.ds(pl.multiple_of(place * width, width), width)],
            land.at[side, sub, core, rows(step)],
            spread_recv.at[landing(step, side, sub, core)],
        )

    def wait_landing(step, part):
        for piece in range(subs):
            for half in range(2):
                spot = land.at[part, piece, half, rows(step)]
                pltpu.make_async_copy(
                    spot, spot, spread_recv.at[landing(step, part, piece, half)]
                ).wait()

    def cross(step):
        return remote(
            land.at[1, :, :, rows(step)],
            crossed.at[:, :, rows(step)],
            cross_send.at[step],
            cross_recv.at[step],
            far,
            place,
        )

    def block(of_rank, step):
        return roll.at[:, pl.ds(of_rank * subs, subs), rows(step)]

    def to_near(of_rank, step):
        return remote(
            block(of_rank, step), block(of_rank, step),
            near_send.at[step], near_recv.at[step], near, place,
        )

    def to_far(of_rank, step):
        return remote(
            block(of_rank, step), block(of_rank, step),
            far_send.at[step], far_recv.at[step], far, place,
        )

    def relay(of_rank, step):
        return remote(
            block(of_rank, step), block(of_rank, step),
            relay_send.at[step], relay_recv.at[step], near, place,
        )

    def roll_out(step):
        return pltpu.make_async_copy(
            roll.at[:, :, rows(step)], rollout.at[:, :, rows(step)], roll_sem.at[step]
        )

    middle = tensor_count // 2
    order = sorted(range(1, tensor_count), key=lambda i: abs(i - middle))

    def issue(step):
        load(step).wait()
        swap(step).wait_recv()
        strip = 16

        @pl.loop(0, chunk // strip)
        def _(i):
            at = pl.ds(pl.multiple_of(step * chunk + i * strip, strip), strip)
            total = mine[at].astype(jnp.float32) + theirs[at].astype(jnp.float32)
            mine[at] = total.astype(mine.dtype)

        for offset in order:
            spread(step, offset).start()

        @pl.when(owner_core == core)
        def _():
            spread_self(step).start()

        @pl.when(owner_core != core)
        def _():
            spread(step, 0).start()

    def issued(step):
        for offset in order:
            spread(step, offset).wait_send()

        @pl.when(owner_core != core)
        def _():
            spread(step, 0).wait_send()

    first_fix = 1.0 - 0.9**10
    second_fix = 1.0 - 0.95**10

    def update(step):
        wait_landing(step, 0)
        cross(step).wait_recv()
        for which in range(3):
            state(which, step).wait()
        strip = 16
        tiles = chunk // strip

        @pl.loop(0, tiles)
        def _(i):
            at = pl.ds(pl.multiple_of(step * chunk + i * strip, strip), strip)
            for half in range(2):
                for piece in range(subs):
                    grad = land[0, piece, half, at].astype(jnp.float32)
                    grad = grad + crossed[piece, half, at].astype(jnp.float32)
                    old = held[0, half, piece, at]
                    moment1 = 0.9 * held[1, half, piece, at] + 0.1 * grad
                    moment2 = 0.95 * held[2, half, piece, at] + 0.05 * grad * grad
                    scaled = jnp.sqrt(moment2 * (1.0 / second_fix)) + 1e-08
                    change = moment1 * (1.0 / first_fix) / scaled + 0.1 * old
                    new = old - 0.003 * change
                    held[0, half, piece, at] = new
                    held[1, half, piece, at] = moment1
                    held[2, half, piece, at] = moment2
                    roll[half, rank * subs + piece, at] = new.astype(roll.dtype)

        to_far(rank, step).start()
        to_near(rank, step).start()
        for which in range(3):
            state_out(which, step).start()

    def pass_on(step):
        to_far(far, step).wait_recv()
        relay(far, step).start()

    def multiply(step):
        to_near(near, step).wait_recv()
        relay(across, step).wait_recv()
        roll_out(step).start()
        for half in range(2):
            weights = roll[half, :, rows(step)].reshape(tensor_count * chunk, width)
            acc[half] += jnp.dot(
                picked[step], weights, preferred_element_type=jnp.float32
            )

    @pl.loop(0, steps)
    def _(step):
        swap(step).start()
        load(step).start()

    token_copy = pltpu.make_async_copy(tokens, token_rows, token_sem)
    for ahead in range(AHEAD):
        issue(ahead)
    token_copy.start()

    @pl.loop(0, steps)
    def _(step):
        for which in range(3):
            state(which, step).start()

    acc[...] = jnp.zeros_like(acc)
    token_copy.wait()
    lanes = lax.broadcasted_iota(jnp.int32, (route.shape[0], token_rows.shape[0]), 1)
    chosen = jnp.where(lanes == route[...], 1.0, 0.0).astype(token_rows.dtype)

    @pl.loop(0, tensor_count)
    def _(part):
        for step in range(steps):
            at = pl.ds(pl.multiple_of(part * slab + step * chunk, chunk), chunk)
            some = jnp.dot(chosen, token_rows[:, at], preferred_element_type=jnp.float32)
            to = pl.ds(pl.multiple_of(part * chunk, chunk), chunk)
            picked[step, :, to] = some.astype(picked.dtype)

    @pl.loop(0, steps + 3)
    def _(now):
        @pl.when((now >= 1) & (now < steps + 1))
        def _():
            update(now - 1)

        @pl.when(now < steps)
        def _():
            wait_landing(now, 1)
            cross(now).start()
            issued(now)

        @pl.when(now < steps - AHEAD)
        def _():
            issue(now + AHEAD)

        @pl.when((now >= 2) & (now < steps + 2))
        def _():
            pass_on(now - 2)

        @pl.when(now >= 3)
        def _():
            multiply(now - 3)

    gate, up = acc[0], acc[1]
    hidden[...] = (gate / (1.0 + jnp.exp(-gate)) * up).astype(hidden.dtype)

    @pl.loop(0, steps)
    def _(step):
        swap(step).wait_send()
        cross(step).wait_send()
        to_far(rank, step).wait_send()
        to_near(rank, step).wait_send()
        relay(far, step).wait_send()
        roll_out(step).wait()
        for which in range(3):
            state_out(which, step).wait()


def entry(tensor_count, grads, s0, s1, s2, tokens, route, o0, o1, o2, *rest):
    kernel(tensor_count, grads, (s0, s1, s2), tokens, route, (o0, o1, o2), *rest)


def fused(grads, master, moment1, moment2, tokens, route):
    tensor_count = lax.axis_size("tensor")
    rank_count = lax.axis_size("dp")
    subs = tensor_count // rank_count
    slab, hidden_width = grads.shape[2:]
    width = hidden_width // tensor_count
    steps = slab // LANES
    routed = route.shape[0]
    split = (2, subs, slab, width)
    states = [array.reshape(split) for array in (master, moment1, moment2)]
    anywhere = pl.BlockSpec(memory_space=pl.ANY)
    vmem = pl.BlockSpec(memory_space=pltpu.VMEM)
    dma = pltpu.SemaphoreType.DMA
    half = jnp.bfloat16
    f32 = jnp.float32
    new_master, new1, new2, rollout, hidden = pl.pallas_call(
        functools.partial(entry, tensor_count),
        out_shape=[jax.ShapeDtypeStruct(split, f32)] * 3
        + [
            jax.ShapeDtypeStruct((2, tensor_count, slab, width), half),
            jax.ShapeDtypeStruct((routed, width), half),
        ],
        in_specs=[anywhere] * 5 + [vmem],
        out_specs=[anywhere] * 4 + [vmem],
        scratch_shapes=[
            pltpu.VMEM((slab, hidden_width), half),
            pltpu.VMEM((slab, hidden_width), half),
            pltpu.VMEM((2, subs, 2, slab, width), half),
            pltpu.VMEM((subs, 2, slab, width), half),
            pltpu.VMEM((3,) + split, f32),
            pltpu.VMEM((2, tensor_count, slab, width), half),
            pltpu.VMEM(tokens.shape, half),
            pltpu.VMEM((steps, routed, tensor_count * LANES), half),
            pltpu.VMEM((2, routed, width), f32),
            dma((steps,)),
            dma((steps,)),
            dma((steps,)),
            dma((3 * steps,)),
            dma,
            dma((steps * tensor_count,)),
            dma((steps * 2 * subs * 2,)),
        ]
        + [dma((steps,))] * 8
        + [dma((3 * steps,)), dma((steps,))],
        compiler_params=pltpu.CompilerParams(
            has_side_effects=True, vmem_limit_bytes=56 * 1024 * 1024
        ),
    )(grads, *states, tokens, route.reshape(routed, 1))
    whole = (2, subs * slab, width)
    return (
        new_master.reshape(whole),
        new1.reshape(whole),
        new2.reshape(whole),
        rollout.reshape(2, tensor_count * slab, width),
        hidden,
    )


def chosen_body(grads, *rest):
    tensor_count, rank_count = lax.axis_size("tensor"), lax.axis_size("dp")
    slab, hidden_width = grads.shape[2:]
    fits = (
        rank_count == 4
        and tensor_count % rank_count == 0
        and slab % LANES == 0
        and slab // LANES > AHEAD
        and hidden_width % (tensor_count * LANES) == 0
    )
    return fused(grads, *rest) if fits else body(grads, *rest)


def solution(mesh):
    in_specs = (
        P("dp", None, "tensor", None),
        P(None, "dp", "tensor"),
        P(None, "dp", "tensor"),
        P(None, "dp", "tensor"),
        P("dp", None),
        P("dp"),
    )
    out_specs = (
        P(None, "dp", "tensor"),
        P(None, "dp", "tensor"),
        P(None, "dp", "tensor"),
        P(None, None, "tensor"),
        P("dp", "tensor"),
    )
    return jax.shard_map(chosen_body, mesh=mesh, in_specs=in_specs, out_specs=out_specs, check_vma=False)
```

```python
import functools

import jax
import jax.numpy as jnp
from jax import lax
from jax.experimental import pallas as pl
from jax.experimental.pallas import tpu as pltpu
from jax.sharding import PartitionSpec as P

MESH = pl.DeviceIdType.MESH
LANES = 128
CHUNK = 64
AHEAD = 4


def body(grads, master, moment1, moment2, tokens, route):
    tensor_count = lax.axis_size("tensor")
    rank_count = lax.axis_size("dp")
    grad_local = grads[0]
    rows_tensor = grad_local.shape[1]
    hidden_width = grad_local.shape[2]
    col_width = hidden_width // tensor_count
    slab = rows_tensor // rank_count
    summed = lax.psum_scatter(grad_local, "dp", scatter_dimension=1, tiled=True).astype(jnp.float32)
    pieces = summed.reshape(2, slab, tensor_count, col_width)
    spread = lax.all_to_all(
        pieces.astype(jnp.bfloat16), "tensor", split_axis=2, concat_axis=1, tiled=True
    ).astype(pieces.dtype)
    spread = spread.reshape(2, rank_count, tensor_count // rank_count, slab, col_width)
    owned = lax.all_to_all(
        spread.astype(jnp.bfloat16), "dp", split_axis=1, concat_axis=3, tiled=True
    ).astype(spread.dtype)
    grad_total = owned.reshape(2, rows_tensor * tensor_count // rank_count, col_width)
    new_moment1 = 0.9 * moment1 + 0.1 * grad_total
    new_moment2 = 0.95 * moment2 + 0.05 * grad_total * grad_total
    first_fix = 1.0 - 0.9**10
    second_fix = 1.0 - 0.95**10
    step_size = (
        new_moment1 / first_fix / (jnp.sqrt(new_moment2 / second_fix) + 1e-08) + 0.1 * master
    )
    new_master = master - 0.003 * step_size
    rollout_shard = new_master.astype(jnp.bfloat16)
    replicated = lax.all_gather(rollout_shard, "dp", axis=1, tiled=True)
    picked = jnp.take(tokens, route, axis=0)
    both = jnp.einsum("rd,kdh->rkh", picked, replicated, preferred_element_type=jnp.float32)
    hidden = (jax.nn.silu(both[:, 0, :]) * both[:, 1, :]).astype(jnp.bfloat16)
    return (new_master, new_moment1, new_moment2, replicated, hidden)


def kernel(
    tensor_count,
    grads,
    states,
    tokens,
    route,
    held,
    roll,
    hidden,
    mine,
    theirs,
    land,
    crossed,
    token_rows,
    picked,
    chosen,
    acc,
    load_sem,
    core_send,
    core_recv,
    state_sem,
    token_sem,
    spread_send,
    spread_recv,
    cross_send,
    cross_recv,
    near_send,
    near_recv,
    far_send,
    far_recv,
    relay_send,
    relay_recv,
):
    rank = lax.axis_index("dp")
    place = lax.axis_index("tensor")
    row, core = rank // 2, rank % 2
    near = row * 2 + 1 - core
    far = (1 - row) * 2 + core
    across = (1 - row) * 2 + 1 - core
    subs = land.shape[1]
    slab = mine.shape[0]
    width = land.shape[4]
    chunk = CHUNK
    steps = slab // chunk
    pairs = slab // LANES
    owner, sub = place // subs, place % subs
    owner_row, owner_core = owner // 2, owner % 2
    side = (owner_row + row) % 2

    def rows(step):
        return pl.ds(pl.multiple_of(step * chunk, chunk), chunk)

    def remote(source, target, send, recv, to_rank, to_place):
        return pltpu.make_async_remote_copy(
            src_ref=source,
            dst_ref=target,
            send_sem=send,
            recv_sem=recv,
            device_id=(to_rank, to_place),
            device_id_type=MESH,
        )

    def load(step):
        return pltpu.make_async_copy(
            grads.at[0, core, rows(step)], mine.at[rows(step)], load_sem.at[step]
        )

    def swap(step):
        return remote(
            grads.at[0, 1 - core, rows(step)],
            theirs.at[rows(step)],
            core_send.at[step],
            core_recv.at[step],
            near,
            place,
        )

    def state(which, step):
        return pltpu.make_async_copy(
            states[which].at[:, :, rows(step)],
            held[which].at[:, :, rows(step)],
            state_sem.at[which * steps + step],
        )

    def landing(step, part, piece, half):
        return ((step * 2 + part) * subs + piece) * 2 + half

    def spread(step, offset):
        goal = (place + offset) % tensor_count
        return remote(
            mine.at[rows(step), pl.ds(pl.multiple_of(goal * width, width), width)],
            land.at[side, sub, core, rows(step)],
            spread_send.at[step * tensor_count + offset],
            spread_recv.at[landing(step, side, sub, core)],
            row * 2 + owner_core,
            goal,
        )

    def spread_self(step):
        return pltpu.make_async_copy(
            mine.at[rows(step), pl.ds(pl.multiple_of(place * width, width), width)],
            land.at[side, sub, core, rows(step)],
            spread_recv.at[landing(step, side, sub, core)],
        )

    def wait_landing(step, part):
        for piece in range(subs):
            for half in range(2):
                spot = land.at[part, piece, half, rows(step)]
                pltpu.make_async_copy(
                    spot, spot, spread_recv.at[landing(step, part, piece, half)]
                ).wait()

    def cross(step):
        return remote(
            land.at[1, :, :, rows(step)],
            crossed.at[:, :, rows(step)],
            cross_send.at[step],
            cross_recv.at[step],
            far,
            place,
        )

    def block(of_rank, step):
        return roll.at[:, pl.ds(of_rank * subs, subs), rows(step)]

    def to_near(of_rank, step):
        return remote(
            block(of_rank, step), block(of_rank, step),
            near_send.at[step], near_recv.at[step], near, place,
        )

    def to_far(of_rank, step):
        return remote(
            block(of_rank, step), block(of_rank, step),
            far_send.at[step], far_recv.at[step], far, place,
        )

    def relay(of_rank, step):
        return remote(
            block(of_rank, step), block(of_rank, step),
            relay_send.at[step], relay_recv.at[step], near, place,
        )

    middle = tensor_count // 2
    order = sorted(range(1, tensor_count), key=lambda i: -abs(i - middle))

    def issue(step):
        load(step).wait()
        swap(step).wait_recv()
        strip = 16

        @pl.loop(0, chunk // strip)
        def _(i):
            at = pl.ds(pl.multiple_of(step * chunk + i * strip, strip), strip)
            total = mine[at].astype(jnp.float32) + theirs[at].astype(jnp.float32)
            mine[at] = total.astype(mine.dtype)

        for offset in order:
            spread(step, offset).start()

        @pl.when(owner_core == core)
        def _():
            spread_self(step).start()

        @pl.when(owner_core != core)
        def _():
            spread(step, 0).start()

    def issued(step):
        for offset in order:
            spread(step, offset).wait_send()

        @pl.when(owner_core != core)
        def _():
            spread(step, 0).wait_send()

    first_fix = 1.0 - 0.9**10
    second_fix = 1.0 - 0.95**10

    def update(step):
        wait_landing(step, 0)
        cross(step).wait_recv()
        for which in range(3):
            state(which, step).wait()
        strip = 16
        tiles = chunk // strip

        @pl.loop(0, tiles)
        def _(i):
            at = pl.ds(pl.multiple_of(step * chunk + i * strip, strip), strip)
            for half in range(2):
                for piece in range(subs):
                    grad = land[0, piece, half, at].astype(jnp.float32)
                    grad = grad + crossed[piece, half, at].astype(jnp.float32)
                    old = held[0][half, piece, at]
                    moment1 = 0.9 * held[1][half, piece, at] + 0.1 * grad
                    moment2 = 0.95 * held[2][half, piece, at] + 0.05 * grad * grad
                    scaled = jnp.sqrt(moment2 * (1.0 / second_fix)) + 1e-08
                    change = moment1 * (1.0 / first_fix) / scaled + 0.1 * old
                    new = old - 0.003 * change
                    held[0][half, piece, at] = new
                    held[1][half, piece, at] = moment1
                    held[2][half, piece, at] = moment2
                    roll[half, rank * subs + piece, at] = new.astype(roll.dtype)

        to_far(rank, step).start()
        to_near(rank, step).start()

    def pass_on(step):
        to_far(far, step).wait_recv()
        relay(far, step).start()

    def multiply(pair):
        for part in range(LANES // chunk):
            step = pair * (LANES // chunk) + part
            to_near(near, step).wait_recv()
            relay(across, step).wait_recv()
        at = pl.ds(pl.multiple_of(pair * LANES, LANES), LANES)
        for half in range(2):
            weights = roll[half, :, at].reshape(tensor_count * LANES, width)
            acc[half] += jnp.dot(
                picked[pair], weights, preferred_element_type=jnp.float32
            )

    def pick(pair):
        for part in range(tensor_count):
            at = pl.ds(pl.multiple_of(part * slab + pair * LANES, LANES), LANES)
            some = jnp.dot(
                chosen[...], token_rows[:, at], preferred_element_type=jnp.float32
            )
            picked[pair, :, part * LANES : (part + 1) * LANES] = some.astype(picked.dtype)

    @pl.loop(0, steps)
    def _(step):
        swap(step).start()
        load(step).start()

    token_copy = pltpu.make_async_copy(tokens, token_rows, token_sem)
    for ahead in range(AHEAD):
        issue(ahead)
    token_copy.start()

    @pl.loop(0, steps)
    def _(step):
        for which in range(3):
            state(which, step).start()

    acc[...] = jnp.zeros_like(acc)
    index = lax.broadcasted_iota(jnp.int32, (token_rows.shape[0], route.shape[1]), 0)
    onehot = jnp.where(index == route[...], 1.0, 0.0)
    chosen[...] = onehot.T.astype(chosen.dtype)
    per = LANES // chunk

    @pl.loop(0, steps + 4)
    def _(now):
        @pl.when(now < steps)
        def _():
            wait_landing(now, 1)
            cross(now).start()
            issued(now)

        @pl.when(now < steps - AHEAD)
        def _():
            issue(now + AHEAD)

        @pl.when(now == 0)
        def _():
            token_copy.wait()

        @pl.when(now < pairs)
        def _():
            pick(now)

        @pl.when((now >= 1) & (now < steps + 1))
        def _():
            update(now - 1)

        @pl.when((now >= 3) & (now < steps + 3))
        def _():
            pass_on(now - 3)

        @pl.when((now >= 4) & ((now - 4) % per == per - 1))
        def _():
            multiply((now - 4) // per)

    gate, up = acc[0], acc[1]
    hidden[...] = (gate / (1.0 + jnp.exp(-gate)) * up).astype(hidden.dtype)

    @pl.loop(0, steps)
    def _(step):
        swap(step).wait_send()
        cross(step).wait_send()
        to_far(rank, step).wait_send()
        to_near(rank, step).wait_send()
        relay(far, step).wait_send()


def entry(tensor_count, grads, s0, s1, s2, tokens, route, o0, o1, o2, *rest):
    kernel(tensor_count, grads, (s0, s1, s2), tokens, route, (o0, o1, o2), *rest)


def fused(grads, master, moment1, moment2, tokens, route):
    tensor_count = lax.axis_size("tensor")
    rank_count = lax.axis_size("dp")
    subs = tensor_count // rank_count
    slab, hidden_width = grads.shape[2:]
    width = hidden_width // tensor_count
    steps = slab // CHUNK
    routed = route.shape[0]
    split = (2, subs, slab, width)
    states = [array.reshape(split) for array in (master, moment1, moment2)]
    anywhere = pl.BlockSpec(memory_space=pl.ANY)
    vmem = pl.BlockSpec(memory_space=pltpu.VMEM)
    dma = pltpu.SemaphoreType.DMA
    half = jnp.bfloat16
    f32 = jnp.float32
    new_master, new1, new2, rollout, hidden = pl.pallas_call(
        functools.partial(entry, tensor_count),
        out_shape=[pltpu.VMEM(split, f32)] * 3
        + [
            pltpu.VMEM((2, tensor_count, slab, width), half),
            pltpu.VMEM((routed, width), half),
        ],
        in_specs=[anywhere] * 5 + [vmem],
        out_specs=[vmem] * 5,
        scratch_shapes=[
            pltpu.VMEM((slab, hidden_width), half),
            pltpu.VMEM((slab, hidden_width), half),
            pltpu.VMEM((2, subs, 2, slab, width), half),
            pltpu.VMEM((subs, 2, slab, width), half),
            pltpu.VMEM(tokens.shape, half),
            pltpu.VMEM((slab // LANES, routed, tensor_count * LANES), half),
            pltpu.VMEM((routed, tokens.shape[0]), half),
            pltpu.VMEM((2, routed, width), f32),
            dma((steps,)),
            dma((steps,)),
            dma((steps,)),
            dma((3 * steps,)),
            dma,
            dma((steps * tensor_count,)),
            dma((steps * 2 * subs * 2,)),
        ]
        + [dma((steps,))] * 8,
        compiler_params=pltpu.CompilerParams(
            has_side_effects=True, vmem_limit_bytes=45 * 1024 * 1024
        ),
    )(grads, *states, tokens, route.reshape(1, routed))
    whole = (2, subs * slab, width)
    return (
        new_master.reshape(whole),
        new1.reshape(whole),
        new2.reshape(whole),
        rollout.reshape(2, tensor_count * slab, width),
        hidden,
    )


def chosen_body(grads, *rest):
    tensor_count, rank_count = lax.axis_size("tensor"), lax.axis_size("dp")
    slab, hidden_width = grads.shape[2:]
    fits = (
        rank_count == 4
        and tensor_count % rank_count == 0
        and slab % LANES == 0
        and slab // CHUNK > AHEAD
        and hidden_width % (tensor_count * LANES) == 0
    )
    return fused(grads, *rest) if fits else body(grads, *rest)


def solution(mesh):
    in_specs = (
        P("dp", None, "tensor", None),
        P(None, "dp", "tensor"),
        P(None, "dp", "tensor"),
        P(None, "dp", "tensor"),
        P("dp", None),
        P("dp"),
    )
    out_specs = (
        P(None, "dp", "tensor"),
        P(None, "dp", "tensor"),
        P(None, "dp", "tensor"),
        P(None, None, "tensor"),
        P("dp", "tensor"),
    )
    return jax.shard_map(chosen_body, mesh=mesh, in_specs=in_specs, out_specs=out_specs, check_vma=False)
```
